256 devices in a mesh: seq: 64 (over z, y, core), head: 4 (over x).
Axes of the slice: x: 4, y: 4, z: 8, core: 2. Of those that a mesh axis runs over, the one named last changes fastest.
Arguments:
- tokens: bfloat16 [8192, 2048], P('seq'), may hold values from -20 to 20, as said below
- projection: bfloat16 [2048, 3072], P(None, 'head'), may hold values from -0.078125 to 0.078125
- context_cotangent: bfloat16 [8192, 2048], P('seq', 'head'), may hold values from -80 to 80
Outputs:
- perturbed_context: bfloat16 [8192, 2048], P('seq', 'head')
- ascent_direction: float32 [2048, 3072], P('seq', 'head')
The draws below stay inside these ranges and needn't reach their ends.
Inputs may be any that keep to these rules, and one draw needn't show every extreme that they name: `tokens`: activations of the layer.
All inputs are finite; a program needn't handle non-finite values.
Results may differ from the reference program's by a relative error of at most 0.017.
Values may be sent and summed in bfloat16 or wider, within the bound.
No kernel may reach another device: no remote copies, remote signals or barrier semaphores. Data moves between devices by JAX's collectives and lax.ppermute only.
A program may use at most 64 MiB of HBM per device.

```python
import math
import jax
import jax.numpy as jnp
from jax import lax

INPUT_FEATURES = 2048
HQ = 16
KEY_VALUE_HEADS = 4
HEAD_DIMENSION = 128
QUERY_PER_GROUP = 4
CW = 3072
SEQUENCE_TOKENS = 8192


def draw_tokens(key, part):
    key_list = jax.random.split(key, 2)
    ramp = 0.7 * 10.0 ** (jnp.arange(INPUT_FEATURES, dtype=jnp.float32) / max(INPUT_FEATURES - 1, 1) - 0.5)
    jitter = jax.random.uniform(key_list[1], (INPUT_FEATURES,), jnp.float32, 0.7, 1.4)
    base = jnp.clip(jax.random.normal(key_list[0], (SEQUENCE_TOKENS, INPUT_FEATURES), jnp.float32), -6.0, 6.0)
    return (base * ramp * jitter).astype(jnp.bfloat16)


def draw_context_cotangent(key, part):
    key_list = jax.random.split(key, 2)
    head_index = (jnp.arange(HQ * HEAD_DIMENSION, dtype=jnp.int32) // HEAD_DIMENSION).astype(jnp.float32)
    head_scale = 0.3 * 10.0 ** (head_index / max(HQ - 1, 1))
    rough = jax.random.uniform(key_list[1], (SEQUENCE_TOKENS, 1), jnp.float32, 0.5, 1.5)
    base = jnp.clip(jax.random.normal(key_list[0], (SEQUENCE_TOKENS, HQ * HEAD_DIMENSION), jnp.float32), -6.0, 6.0)
    return (base * rough * head_scale).astype(jnp.bfloat16)


def levels(key, dims, cuts, low, top_value):
    def one(position, blocks):
        heights = jax.random.uniform(jax.random.fold_in(jax.random.fold_in(key, 6), position), (blocks,), jnp.float32, low / len(cuts), top_value / len(cuts))
        return jnp.repeat(jnp.exp(heights), dims[position] // blocks).reshape((-1,) + (1,) * (len(dims) - position - 1))

    level = one(*cuts[0])
    for cut in cuts[1:]:
        level = level * one(*cut)
    return level


def noise(stream_key, dims, scale, bound, pieces=(), held_as=jnp.bfloat16):
    entries = jax.random.normal(stream_key, dims, jnp.float32) * scale
    if len(pieces) > 0:
        entries = levels(stream_key, dims, pieces, -0.22, 0.18) * entries
    return jnp.clip(entries, min=-bound, max=bound).astype(held_as)


def setup_inputs(seed: int = 0) -> dict:
    key_of = jax.random.split(jax.random.key(seed), 4)
    return {
        "tokens": draw_tokens(jax.random.fold_in(key_of[3], 71), 0),
        "projection": noise(key_of[1], (INPUT_FEATURES, CW), (INPUT_FEATURES * 3) ** -0.5, 0.078125, ((1, 4),)),
        "context_cotangent": draw_context_cotangent(jax.random.fold_in(key_of[3], 71), 0),
    }


masked_score = -1e+30

def rounded(values):
    return lax.optimization_barrier(values.astype(jnp.bfloat16)).astype(jnp.float32)

def split_heads(projected_weight):
    reshaped_grads = projected_weight.reshape(projected_weight.shape[0], KEY_VALUE_HEADS, QUERY_PER_GROUP + 2, HEAD_DIMENSION)
    query = jnp.moveaxis(reshaped_grads[:, :, :QUERY_PER_GROUP], 1, 0)
    key_rows = jnp.moveaxis(reshaped_grads[:, :, QUERY_PER_GROUP], 1, 0)
    value_rows = jnp.moveaxis(reshaped_grads[:, :, QUERY_PER_GROUP + 1], 1, 0)
    return (query, key_rows, value_rows)

def block_scores(query_block, key_rows, positions):
    scores = jnp.einsum('tgd,kd->tgk', query_block.astype(jnp.float32), key_rows.astype(jnp.float32)) * HEAD_DIMENSION ** (-0.5)
    key_pos = jnp.arange(key_rows.shape[0], dtype=jnp.int32)
    allowed = key_pos[None, None, :] <= positions[:, None, None]
    return jnp.where(allowed, scores, masked_score)

def forward_group(query, key_rows, value_rows):
    query_span = min(512, SEQUENCE_TOKENS)
    count_blocks = SEQUENCE_TOKENS // query_span
    blocks = query.reshape(count_blocks, query_span, QUERY_PER_GROUP, HEAD_DIMENSION)

    def per_block(inputs):
        block_index, query_block = inputs
        positions = block_index * query_span + jnp.arange(query_span, dtype=jnp.int32)
        scores = block_scores(query_block, key_rows, positions)
        row_max = lax.optimization_barrier(jnp.max(scores, axis=-1, keepdims=True))
        weights = jnp.exp(scores - row_max)
        row_total = lax.optimization_barrier(jnp.sum(weights, axis=-1, keepdims=True))
        context = jnp.einsum('tgk,kd->tgd', weights, value_rows.astype(jnp.float32), precision=lax.Precision.HIGHEST) / row_total
        return (context.astype(jnp.bfloat16), (row_max + jnp.log(row_total))[..., 0])
    context, log_total = lax.map(per_block, (jnp.arange(count_blocks, dtype=jnp.int32), blocks))
    return (context.reshape(SEQUENCE_TOKENS, QUERY_PER_GROUP, HEAD_DIMENSION), log_total.reshape(SEQUENCE_TOKENS, QUERY_PER_GROUP))

def backward_group(query, key_rows, value_rows, context, log_total, grad_out):
    query_span = min(512, SEQUENCE_TOKENS)
    count_blocks = SEQUENCE_TOKENS // query_span
    score_scale = HEAD_DIMENSION ** (-0.5)
    row_delta = lax.optimization_barrier(jnp.sum(grad_out.astype(jnp.float32) * context.astype(jnp.float32), axis=-1))
    keys_f = key_rows.astype(jnp.float32)
    values_f = value_rows.astype(jnp.float32)

    def per_block(carry, inputs):
        key_grad, value_grad = carry
        block_index, query_block, grad_block, lse_block, delta_block = inputs
        positions = block_index * query_span + jnp.arange(query_span, dtype=jnp.int32)
        scores = block_scores(query_block, key_rows, positions)
        probs_full = jnp.exp(scores - lse_block[..., None])
        grad_f = grad_block.astype(jnp.float32)
        prob_grad = jnp.einsum('tgd,kd->tgk', grad_f, values_f)
        score_grad = rounded(probs_full * (prob_grad - delta_block[..., None]) * score_scale)
        query_grad = jnp.einsum('tgk,kd->tgd', score_grad, keys_f).astype(jnp.bfloat16)
        key_grad = key_grad + jnp.einsum('tgk,tgd->kd', score_grad, query_block.astype(jnp.float32))
        value_grad = value_grad + jnp.einsum('tgk,tgd->kd', rounded(probs_full), grad_f)
        return ((key_grad, value_grad), query_grad)
    initial = (jnp.zeros((SEQUENCE_TOKENS, HEAD_DIMENSION), jnp.float32), jnp.zeros((SEQUENCE_TOKENS, HEAD_DIMENSION), jnp.float32))
    inputs = (jnp.arange(count_blocks, dtype=jnp.int32), query.reshape(count_blocks, query_span, QUERY_PER_GROUP, HEAD_DIMENSION), grad_out.reshape(count_blocks, query_span, QUERY_PER_GROUP, HEAD_DIMENSION), log_total.reshape(count_blocks, query_span, QUERY_PER_GROUP), row_delta.reshape(count_blocks, query_span, QUERY_PER_GROUP))
    (key_grad, value_grad), query_grad = lax.scan(per_block, initial, inputs)
    return (query_grad.reshape(SEQUENCE_TOKENS, QUERY_PER_GROUP, HEAD_DIMENSION), key_grad.astype(jnp.bfloat16), value_grad.astype(jnp.bfloat16))

def reference(tokens, projection, context_cotangent):
    projected_weight = jnp.dot(tokens, projection, preferred_element_type=jnp.float32).astype(jnp.bfloat16)
    query, key_rows, value_rows = split_heads(projected_weight)
    gradient_by_group = jnp.moveaxis(context_cotangent.reshape(SEQUENCE_TOKENS, KEY_VALUE_HEADS, QUERY_PER_GROUP, HEAD_DIMENSION), 1, 0)

    def group_pass(inputs):
        query_one, key_one, value_one, grad_one = inputs
        context, log_total = forward_group(query_one, key_one, value_one)
        return backward_group(query_one, key_one, value_one, context, log_total, grad_one)
    query_grad, key_grad, value_grad = lax.map(group_pass, (query, key_rows, value_rows, gradient_by_group))
    head_grads = jnp.concatenate([jnp.moveaxis(query_grad, 0, 1), jnp.moveaxis(key_grad, 0, 1)[:, :, None, :], jnp.moveaxis(value_grad, 0, 1)[:, :, None, :]], axis=2).reshape(SEQUENCE_TOKENS, CW)
    weight_grad = jnp.dot(tokens.T, head_grads, preferred_element_type=jnp.float32)
    grad_norm = jnp.sqrt(jnp.sum(weight_grad * weight_grad))
    direction = weight_grad * (math.sqrt(INPUT_FEATURES * CW) / grad_norm)
    moved_weights = (projection.astype(jnp.float32) + 0.2 * math.sqrt(CW) / grad_norm * weight_grad).astype(jnp.bfloat16)
    projected_new = jnp.dot(tokens, moved_weights, preferred_element_type=jnp.float32).astype(jnp.bfloat16)
    query_new, key_new, value_new = split_heads(projected_new)

    def forward_only(inputs):
        return forward_group(inputs[0], inputs[1], inputs[2])[0]
    context_new = lax.map(forward_only, (query_new, key_new, value_new))
    perturbed = jnp.moveaxis(context_new, 0, 1).reshape(SEQUENCE_TOKENS, HQ * HEAD_DIMENSION)
    return (perturbed, direction)
```

```python
import math

import jax
import jax.numpy as jnp
from jax import lax
from jax.experimental import pallas as pl
from jax.experimental.pallas import tpu as pltpu
from jax.sharding import Mesh
from jax.sharding import PartitionSpec as P


FEATURES = 2048
GROUPS = 4
D = 128
HQ = 4
ROWS = 128
NY = 4
NC = 2
NZ = 8
NQ = NY * NC
SCALE = D ** (-0.5)
SCALE2 = SCALE * math.log2(math.e)
MASKED = -1e30
FLOOR = -1e29
F32 = jnp.float32
BF16 = jnp.bfloat16
NT = (((1,), (1,)), ((), ()))
NN = (((1,), (0,)), ((), ()))


def shift(x, axis, size, step):
    return lax.ppermute(x, axis, [(j, (j + step) % size) for j in range(size)])


def swap(x):
    return shift(x, "c", NC, 1)


def pieces(x, axis, size):
    return [x] + [shift(x, axis, size, s) for s in range(1, size)]


def gather_yc(x):
    mine = pieces(x, "y", NY)
    return mine + [swap(m) for m in mine]


def sum_to_owner(terms, axis, size):
    total = terms[0].astype(F32)
    for s in range(1, size):
        total = total + shift(terms[s].astype(BF16), axis, size, -s).astype(F32)
    return total


def scatter_yc(mine, partner):
    total = mine + swap(partner).astype(F32)
    return sum_to_owner([total[s] for s in range(NY)], "y", NY)


def dot(a, b, dims):
    return lax.dot_general(a, b, dims, preferred_element_type=F32)


def tile_limits(where, a):
    y, c = where[1], where[2]
    lane = lax.broadcasted_iota(jnp.int32, (1, 2 * ROWS), 1)

    def limit(slot):
        other = ((y - slot % NY + NY) % NY) * NC + (c + slot // NY) % NC
        return jnp.where(other > y * NC + c, ROWS, -1)

    first = jnp.where(a == 0, lane, limit(2 * a))
    return jnp.where(lane < ROWS, first, limit(2 * a + 1))


def pair(ref, a, h):
    block = ref[pl.ds(2 * a, 2), :, pl.ds(pl.multiple_of(h * D, D), D)]
    return block.reshape(2 * ROWS, D)


def slot_scores(kv, s, q, limits):
    scores = dot(kv[s][:, :D], q, NT) * SCALE2
    if s == 0:
        row = lax.broadcasted_iota(jnp.int32, scores.shape, 0)
        scores = jnp.where(row <= limits, scores, MASKED)
    return scores


def slot_bias(where, s):
    if s == 0:
        return jnp.float32(0.0)
    return jnp.where(s <= where[0], jnp.float32(0.0), jnp.float32(MASKED))


def row_weights(where, kv, q, limits):
    scores = [slot_scores(kv, s, q, limits) for s in range(NZ)]
    bias = [slot_bias(where, s) for s in range(NZ)]
    top = jnp.full((1, 2 * ROWS), FLOOR, F32)
    for s in range(NZ):
        top = jnp.maximum(top, jnp.max(scores[s], axis=0, keepdims=True) + bias[s])
    weights = [jnp.exp2(scores[s] - (top - bias[s])) for s in range(NZ)]
    total = sum(jnp.sum(w, axis=0, keepdims=True) for w in weights)
    safe = jnp.maximum(total, 1e-30)
    lse = jnp.where(total > 0.0, top + jnp.log2(safe), MASKED)
    return weights, safe, lse


def put_rows(ref, a, h, row):
    ref[2 * a, pl.ds(h, 1), :] = row[:, :ROWS]
    ref[2 * a + 1, pl.ds(h, 1), :] = row[:, ROWS:]


def take_rows(ref, a, h):
    rows = [ref[2 * a + j, pl.ds(h, 1), :] for j in range(2)]
    return jnp.concatenate(rows, axis=1)


def fill(scratch, refs):
    for s, ref in enumerate(refs):
        scratch[s] = ref[...]


def put_tile(mine_ref, partner_ref, a, h, out):
    rows = pl.ds(pl.multiple_of(h * D, D), D)

    def put(ref, b):
        ref[b, rows, :] = out[:, :ROWS].astype(ref.dtype)
        ref[b + 1, rows, :] = out[:, ROWS:].astype(ref.dtype)

    @pl.when(a < 2)
    def _():
        put(mine_ref, 2 * a)

    @pl.when(a >= 2)
    def _():
        put(partner_ref, 2 * a - NY)


def stats_kernel(where, *refs):
    qg_refs, kv = refs[:NQ], refs[NQ : NQ + NZ]
    out_ref, qg_all = refs[NQ + NZ :]
    fill(qg_all, qg_refs)

    def tile(i, carry):
        h, a = i // NY, i % NY
        q = pair(qg_all, a, h)
        g = pair(qg_all, a, HQ + h)
        weights, safe, lse = row_weights(where, kv, q, tile_limits(where, a))
        acc = jnp.zeros((1, 2 * ROWS), F32)
        for s in range(NZ):
            prob_grad = dot(kv[s][:, D:], g, NT)
            acc = acc + jnp.sum(weights[s] * prob_grad, axis=0, keepdims=True)
        put_rows(out_ref, a, h, lse)
        put_rows(out_ref, a, HQ + h, acc / safe)
        return carry

    lax.fori_loop(0, HQ * NY, tile, 0)


def merged_rows(parts):
    top = parts[0][0]
    for lse, _ in parts[1:]:
        top = jnp.maximum(top, lse)
    weights = [jnp.exp2(lse - top) for lse, _ in parts]
    total = sum(weights)
    value = sum(w * v for w, (_, v) in zip(weights, parts)) / total
    return top + jnp.log2(total), value


def pair_kernel(own, got, out_ref):
    for slot in range(NQ):
        other = (slot + NY) % NQ
        lse, delta = merged_rows(
            [(r[k, :HQ, :], r[k, HQ:, :]) for r, k in ((own, slot), (got, other))]
        )
        out_ref[slot, :HQ, :] = lse
        out_ref[slot, HQ:, :] = delta


def forward_kernel(where, *refs):
    q_refs, kv = refs[:NQ], refs[NQ : NQ + NZ]
    mine_ref, partner_ref, lse_ref, q_all, vt = refs[NQ + NZ :]
    fill(q_all, q_refs)
    for s in range(NZ):
        vt[:, s * ROWS : (s + 1) * ROWS] = kv[s][:, D:].T
    lse_ref[...] = jnp.zeros(lse_ref.shape, F32)

    def tile(i, carry):
        h, a = i // NY, i % NY
        q = pair(q_all, a, h)
        weights, safe, lse = row_weights(where, kv, q, tile_limits(where, a))
        p = jnp.concatenate([w.astype(BF16) for w in weights], axis=0)
        put_tile(mine_ref, partner_ref, a, h, dot(vt[...], p, NN) * (1.0 / safe))
        put_rows(lse_ref, a, h, lse)
        return carry

    lax.fori_loop(0, HQ * NY, tile, 0)
    for b in range(NY):
        partner_ref[b, HQ * D :, :] = packed(lse_ref[NY + b, :HQ, :])


def packed(rows):
    high = rows.astype(BF16)
    rest = rows - high.astype(F32)
    middle = rest.astype(BF16)
    low = (rest - middle.astype(F32)).astype(BF16)
    return jnp.concatenate([high, middle, low, jnp.zeros_like(low)], axis=0)


def unpacked(tile):
    rows = tile.astype(F32)
    return rows[:HQ] + rows[HQ : 2 * HQ] + rows[2 * HQ : 3 * HQ]


def join_kernel(mine, lse_ref, got, *outs):
    for b in range(NY):
        ours, theirs = lse_ref[b, :HQ, :], unpacked(got[b, HQ * D :, :])
        top = jnp.maximum(ours, theirs)
        first, second = jnp.exp2(ours - top), jnp.exp2(theirs - top)
        total = first + second
        first, second = first / total, second / total
        lse = top + jnp.log2(total)
        out = outs[b]
        for h in range(HQ):
            rows = slice(h * D, (h + 1) * D)
            value = mine[b, rows, :] * first[h : h + 1] + got[b, rows, :].astype(F32) * second[
                h : h + 1
            ]
            out[rows, :] = value.astype(out.dtype)
        if b == 0:
            outs[NY][...] = jnp.concatenate([lse, lse], axis=0)
        else:
            out[HQ * D :, :] = packed(lse)


def last_kernel(own, lse_ref, *refs):
    others, out_ref = refs[: NY - 1], refs[NY - 1]
    lses = [lse_ref[:HQ, :]] + [unpacked(r[HQ * D :, :]) for r in others]
    top = lses[0]
    for lse in lses[1:]:
        top = jnp.maximum(top, lse)
    weights = [jnp.exp2(lse - top) for lse in lses]
    total = sum(weights)
    weights = [w / total for w in weights]
    for h in range(HQ):
        rows = slice(h * D, (h + 1) * D)
        value = own[rows, :] * weights[0][h : h + 1]
        for r, w in zip(others, weights[1:]):
            value = value + r[rows, :].astype(F32) * w[h : h + 1]
        out_ref[:, rows] = value.T.astype(out_ref.dtype)


def backward_kernel(where, *refs):
    qg_refs, kv, refs = refs[:NQ], refs[NQ : NQ + NZ], refs[NQ + NZ :]
    stats, (mine_ref, partner_ref), refs = refs[:NY], refs[NY : NY + 2], refs[NY + 2 :]
    kv_refs, (qg_all, rows_ref, kt, dk, dv) = refs[:NZ], refs[NZ:]
    fill(qg_all, qg_refs)
    for s in range(NZ):
        kt[:, s * ROWS : (s + 1) * ROWS] = kv[s][:, :D].T
    for slot in range(NQ):
        parts = []
        for s in range(NY):
            k = slot - slot % NY + (slot - s) % NY
            parts.append((stats[s][k, :HQ, :], stats[s][k, HQ:, :]))
        lse, delta = merged_rows(parts)
        rows_ref[slot, :HQ, :] = lse
        rows_ref[slot, HQ:, :] = delta
    dk[...] = jnp.zeros(dk.shape, F32)
    dv[...] = jnp.zeros(dv.shape, F32)

    def tile(i, carry):
        h, a = i // NY, i % NY
        q = pair(qg_all, a, h)
        g = pair(qg_all, a, HQ + h)
        lse = take_rows(rows_ref, a, h)
        delta = take_rows(rows_ref, a, HQ + h)
        limits = tile_limits(where, a)
        probs, grads = [], []
        for s in range(NZ):
            scores = slot_scores(kv, s, q, limits)
            p = jnp.exp2(scores - (lse - slot_bias(where, s)))
            prob_grad = dot(kv[s][:, D:], g, NT)
            probs.append(p.astype(BF16))
            grads.append((p * (prob_grad - delta)).astype(BF16))
        p = jnp.concatenate(probs, axis=0)
        ds = jnp.concatenate(grads, axis=0)
        dv[...] += dot(p, g, NN)
        dk[...] += dot(ds, q, NN)
        put_tile(mine_ref, partner_ref, a, h, dot(kt[...], ds, NN) * SCALE)
        return carry

    lax.fori_loop(0, HQ * NY, tile, 0)
    for s in range(NZ):
        ref = kv_refs[s]
        rows = slice(s * ROWS, (s + 1) * ROWS)
        ref[:, :D] = (dk[rows, :] * SCALE).astype(ref.dtype)
        ref[:, D:] = dv[rows, :].astype(ref.dtype)


SHARE = FEATURES // (NZ * NQ)
WIDTH = (HQ + 2) * D


def projection_kernel(tokens_ref, weights_ref, grad_ref, out_ref, heads_ref, kv_ref):
    out = dot(tokens_ref[...], weights_ref[...], NN)
    out_ref[...] = out
    heads_ref[:, : HQ * D] = out[:, : HQ * D].astype(BF16)
    heads_ref[:, HQ * D :] = grad_ref[...]
    kv_ref[...] = out[:, HQ * D :].astype(BF16)


def feature_kernel(where, tokens_ref, *refs):
    outs, by_owner = refs[:NY], refs[NY]
    y, c = where[1], where[2]
    for k in range(NQ):
        cols = [
            tokens_ref[:, (j * NQ + k) * SHARE : (j * NQ + k + 1) * SHARE] for j in range(NZ)
        ]
        by_owner[k] = jnp.concatenate(cols, axis=1)
    for s in range(NY):
        row = (y + s) % NY
        outs[s][0] = by_owner[row * NC + c]
        outs[s][1] = by_owner[row * NC + 1 - c]


def feature_slot(refs, slot):
    return refs[slot][slot // NY]


def weight_kernel(where, *refs):
    features, hq, hkv = refs[:NQ], refs[NQ : 2 * NQ], refs[2 * NQ : 3 * NQ]
    outs, (t_all, h_all, grad) = refs[3 * NQ : 3 * NQ + NZ], refs[3 * NQ + NZ :]
    for slot in range(NQ):
        cols = slice(slot * ROWS, (slot + 1) * ROWS)
        t_all[cols, :] = feature_slot(features, slot)
        h_all[: HQ * D, cols] = hq[slot][...]
        h_all[HQ * D :, cols] = hkv[slot][...].T
    for k in range(HQ + 2):
        rows = slice(k * D, (k + 1) * D)
        grad[:, rows] = dot(h_all[rows, :], t_all[...], NN).T
    for s in range(NZ):
        row = (where[0] - s + NZ) % NZ
        rows = grad[pl.ds(pl.multiple_of(row * SHARE, SHARE), SHARE), :]
        outs[s][...] = rows.astype(outs[s].dtype)


def moved_kernel(where, *refs):
    features, shares = refs[:NQ], refs[NQ : NQ + NZ]
    mine_ref, partner_ref, squares_ref, rows_ref = refs[NQ + NZ :]
    squares = jnp.zeros((8, WIDTH), F32)
    for s in range(NZ):
        row = (where[0] - s + NZ) % NZ
        rows_ref[pl.ds(pl.multiple_of(row * SHARE, SHARE), SHARE), :] = shares[s][...]
        value = jnp.square(shares[s][...].astype(F32))
        for k in range(SHARE // 8):
            squares = squares + value[8 * k : 8 * k + 8]
    squares_ref[...] = jnp.full(squares_ref.shape, jnp.sum(squares), F32)
    for b in range(NY):
        mine_ref[b] = dot(feature_slot(features, b), rows_ref[...], NN)
        partner_ref[b] = dot(feature_slot(features, NY + b), rows_ref[...], NN).astype(BF16)


def call(kernel, outs, scratch, matmuls, *args):
    vmem = pl.BlockSpec(memory_space=pltpu.VMEM)
    smem = pl.BlockSpec(memory_space=pltpu.SMEM)
    specs = [smem if a.dtype == jnp.int32 else vmem for a in args]
    size = HQ * NQ * ROWS * NZ * ROWS
    work = 2 * matmuls * size * D + (8 * size if matmuls else size)
    return pl.pallas_call(
        kernel,
        out_shape=outs,
        in_specs=specs,
        out_specs=jax.tree.map(lambda _: vmem, outs),
        scratch_shapes=scratch,
        cost_estimate=pl.CostEstimate(
            flops=work, bytes_accessed=1 << 20, transcendentals=size if matmuls else 0
        ),
        compiler_params=pltpu.CompilerParams(vmem_limit_bytes=48 << 20),
    )(*args)


def shaped(dtype, *dims):
    return jax.ShapeDtypeStruct(dims, dtype)


def on_device(tokens, projection, context_cotangent):
    z, y, c = lax.axis_index("z"), lax.axis_index("y"), lax.axis_index("c")
    where = jnp.stack([z, y, c]).astype(jnp.int32)
    rows_all = pltpu.VMEM((NQ, ROWS, HQ * D), BF16)
    both_all = pltpu.VMEM((NQ, ROWS, 2 * HQ * D), BF16)
    keys_all = pltpu.VMEM((D, NZ * ROWS), BF16)
    key_sums = pltpu.VMEM((NZ * ROWS, D), F32)
    stat = shaped(F32, NQ, 2 * HQ, ROWS)

    projected, heads, key_value = call(
        projection_kernel,
        (shaped(F32, ROWS, WIDTH), shaped(BF16, ROWS, 2 * HQ * D), shaped(BF16, ROWS, 2 * D)),
        (),
        0,
        tokens,
        projection,
        context_cotangent,
    )
    key_value = pieces(key_value, "z", NZ)
    heads = gather_yc(heads)

    features = call(
        feature_kernel,
        tuple(shaped(BF16, NC, ROWS, FEATURES // NQ) for _ in range(NY)),
        (pltpu.VMEM((NQ, ROWS, FEATURES // NQ), BF16),),
        0,
        where,
        tokens,
    )
    features = [features[0]] + [shift(features[s], "y", NY, s) for s in range(1, NY)]
    features = features + [swap(f) for f in features]

    stats = call(
        stats_kernel, stat, (both_all,), 2, where, *heads, *key_value
    )
    stats = call(pair_kernel, stat, (), 0, stats, swap(stats))
    stats = pieces(stats, "y", NY)

    outs = (
        shaped(F32, NY, HQ * D, ROWS),
        shaped(BF16, NY, HQ * D, ROWS),
        shaped(F32, ROWS, 2 * D),
    ) + tuple(shaped(BF16, ROWS, 2 * D) for _ in range(NZ - 1))
    mine, partner, *kv_terms = call(
        backward_kernel,
        outs,
        (both_all, pltpu.VMEM((NQ, 2 * HQ, ROWS), F32), keys_all, key_sums, key_sums),
        5,
        where,
        *heads,
        *key_value,
        *stats,
    )
    query_grad = gather_yc(scatter_yc(mine, partner).astype(BF16))
    key_value_grad = gather_yc(sum_to_owner(kv_terms, "z", NZ).astype(BF16))

    grad_terms = call(
        weight_kernel,
        (shaped(F32, SHARE, WIDTH),) + tuple(shaped(BF16, SHARE, WIDTH) for _ in range(NZ - 1)),
        (
            pltpu.VMEM((NQ * ROWS, FEATURES // NQ), BF16),
            pltpu.VMEM((WIDTH, NQ * ROWS), BF16),
            pltpu.VMEM((FEATURES // NQ, WIDTH), F32),
        ),
        0,
        where,
        *features,
        *query_grad,
        *key_value_grad,
    )
    own_grad = sum_to_owner(grad_terms, "z", NZ)

    mine, partner, squares = call(
        moved_kernel,
        (
            shaped(F32, NY, ROWS, WIDTH),
            shaped(BF16, NY, ROWS, WIDTH),
            shaped(F32, 8, 128),
        ),
        (pltpu.VMEM((FEATURES // NQ, WIDTH), BF16),),
        0,
        where,
        *features,
        *pieces(own_grad.astype(BF16), "z", NZ),
    )
    moved_rows = scatter_yc(mine, partner)
    squares = squares + swap(squares)
    squares = sum(pieces(squares, "y", NY))
    squares = sum(pieces(squares, "head", GROUPS))
    grad_norm = jnp.sqrt(squares[0, 0])

    width = GROUPS * WIDTH
    direction = own_grad * (math.sqrt(FEATURES * width) / grad_norm)
    projected_new = projected + (0.2 * math.sqrt(width) / grad_norm) * moved_rows

    projected_new = projected_new.astype(BF16)
    key_value_new = pieces(projected_new[:, HQ * D :], "z", NZ)
    query_new = gather_yc(projected_new[:, : HQ * D])
    pack = HQ * D + 4 * HQ
    mine, partner, lse = call(
        forward_kernel,
        (shaped(F32, NY, HQ * D, ROWS), shaped(BF16, NY, pack, ROWS), stat),
        (rows_all, keys_all),
        2,
        where,
        *query_new,
        *key_value_new,
    )
    own, *others, lse = call(
        join_kernel,
        (shaped(F32, HQ * D, ROWS),)
        + tuple(shaped(BF16, pack, ROWS) for _ in range(NY - 1))
        + (shaped(F32, 2 * HQ, ROWS),),
        (),
        0,
        mine,
        lse,
        swap(partner),
    )
    others = [shift(others[s - 1], "y", NY, -s) for s in range(1, NY)]
    perturbed = call(last_kernel, shaped(BF16, ROWS, HQ * D), (), 0, own, lse, *others)
    return (perturbed, direction)


def solution(mesh):
    finer = Mesh(mesh.devices.reshape(NZ, NY, NC, GROUPS), ("z", "y", "c", "head"))
    seq = ("z", "y", "c")

    return jax.shard_map(
        on_device,
        mesh=finer,
        in_specs=(P(seq, None), P(None, "head"), P(seq, "head")),
        out_specs=(P(seq, "head"), P(seq, "head")),
        check_vma=False,
    )
```

```python
import math

import jax
import jax.numpy as jnp
from jax import lax
from jax.experimental import pallas as pl
from jax.experimental.pallas import tpu as pltpu
from jax.sharding import Mesh
from jax.sharding import PartitionSpec as P


FEATURES = 2048
GROUPS = 4
D = 128
HQ = 4
ROWS = 128
NY = 4
NC = 2
NZ = 8
NQ = NY * NC
SCALE = D ** (-0.5)
SCALE2 = SCALE * math.log2(math.e)
MASKED = -1e30
FLOOR = -1e29
F32 = jnp.float32
BF16 = jnp.bfloat16
NT = (((1,), (1,)), ((), ()))
NN = (((1,), (0,)), ((), ()))


def shift(x, axis, size, step):
    return lax.ppermute(x, axis, [(j, (j + step) % size) for j in range(size)])


def swap(x):
    return shift(x, "c", NC, 1)


def pieces(x, axis, size):
    return [x] + [shift(x, axis, size, s) for s in range(1, size)]


def gather_yc(x):
    mine = pieces(x, "y", NY)
    return mine + [swap(m) for m in mine]


def sum_to_owner(terms, axis, size):
    total = terms[0].astype(F32)
    for s in range(1, size):
        total = total + shift(terms[s].astype(BF16), axis, size, -s).astype(F32)
    return total


def scatter_yc(mine, partner):
    total = mine + swap(partner).astype(F32)
    return sum_to_owner([total[s] for s in range(NY)], "y", NY)


def dot(a, b, dims):
    return lax.dot_general(a, b, dims, preferred_element_type=F32)


def tile_limits(where, a):
    y, c = where[1], where[2]
    lane = lax.broadcasted_iota(jnp.int32, (1, 2 * ROWS), 1)

    def limit(slot):
        other = ((y - slot % NY + NY) % NY) * NC + (c + slot // NY) % NC
        return jnp.where(other > y * NC + c, ROWS, -1)

    first = jnp.where(a == 0, lane, limit(2 * a))
    return jnp.where(lane < ROWS, first, limit(2 * a + 1))


def pair(ref, a, h):
    block = ref[pl.ds(2 * a, 2), :, pl.ds(pl.multiple_of(h * D, D), D)]
    return block.reshape(2 * ROWS, D)


def slot_scores(kv, s, q, limits):
    scores = dot(kv[s][:, :D], q, NT) * SCALE2
    if s == 0:
        row = lax.broadcasted_iota(jnp.int32, scores.shape, 0)
        scores = jnp.where(row <= limits, scores, MASKED)
    return scores


def slot_bias(where, s):
    if s == 0:
        return jnp.float32(0.0)
    return jnp.where(s <= where[0], jnp.float32(0.0), jnp.float32(MASKED))


def slot_weights(where, kv, s, q, limits):
    scores = slot_scores(kv, s, q, limits)
    top = jnp.maximum(jnp.max(scores, axis=0, keepdims=True), FLOOR)
    weights = jnp.exp2(scores - top)
    total = jnp.sum(weights, axis=0, keepdims=True)
    return weights, total, top + slot_bias(where, s)


def slot_factors(tops, totals):
    top = tops[0]
    for t in tops[1:]:
        top = jnp.maximum(top, t)
    factors = [jnp.exp2(t - top) for t in tops]
    total = sum(f * t for f, t in zip(factors, totals))
    safe = jnp.maximum(total, 1e-30)
    lse = jnp.where(total > 0.0, top + jnp.log2(safe), MASKED)
    inverse = 1.0 / safe
    return [f * inverse for f in factors], lse


def put_rows(ref, a, h, row):
    ref[2 * a, pl.ds(h, 1), :] = row[:, :ROWS]
    ref[2 * a + 1, pl.ds(h, 1), :] = row[:, ROWS:]


def take_rows(ref, a, h):
    rows = [ref[2 * a + j, pl.ds(h, 1), :] for j in range(2)]
    return jnp.concatenate(rows, axis=1)


def fill(scratch, refs):
    for s, ref in enumerate(refs):
        scratch[s] = ref[...]


def put_tile(mine_ref, partner_ref, a, h, out):
    rows = pl.ds(pl.multiple_of(h * D, D), D)

    def put(ref, b):
        ref[b, rows, :] = out[:, :ROWS].astype(ref.dtype)
        ref[b + 1, rows, :] = out[:, ROWS:].astype(ref.dtype)

    @pl.when(a < 2)
    def _():
        put(mine_ref, 2 * a)

    @pl.when(a >= 2)
    def _():
        put(partner_ref, 2 * a - NY)


def stats_kernel(where, *refs):
    qg_refs, kv = refs[:NQ], refs[NQ : NQ + NZ]
    out_ref, qg_all = refs[NQ + NZ :]
    fill(qg_all, qg_refs)

    def tile(i, carry):
        h, a = i // NY, i % NY
        q = pair(qg_all, a, h)
        g = pair(qg_all, a, HQ + h)
        limits = tile_limits(where, a)
        tops, totals, values = [], [], []
        for s in range(NZ):
            weights, total, top = slot_weights(where, kv, s, q, limits)
            prob_grad = dot(kv[s][:, D:], g, NT)
            values.append(jnp.sum(weights * prob_grad, axis=0, keepdims=True))
            tops.append(top)
            totals.append(total)
        factors, lse = slot_factors(tops, totals)
        put_rows(out_ref, a, h, lse)
        put_rows(out_ref, a, HQ + h, sum(f * v for f, v in zip(factors, values)))
        return carry

    lax.fori_loop(0, HQ * NY, tile, 0, unroll=4)


def merged_rows(parts):
    top = parts[0][0]
    for lse, _ in parts[1:]:
        top = jnp.maximum(top, lse)
    weights = [jnp.exp2(lse - top) for lse, _ in parts]
    total = sum(weights)
    value = sum(w * v for w, (_, v) in zip(weights, parts)) / total
    return top + jnp.log2(total), value


def pair_kernel(own, got, out_ref):
    for slot in range(NQ):
        other = (slot + NY) % NQ
        lse, delta = merged_rows(
            [(r[k, :HQ, :], r[k, HQ:, :]) for r, k in ((own, slot), (got, other))]
        )
        out_ref[slot, :HQ, :] = lse
        out_ref[slot, HQ:, :] = delta


def forward_kernel(where, *refs):
    q_refs, kv = refs[:NQ], refs[NQ : NQ + NZ]
    mine_ref, partner_ref, lse_ref, q_all, vt = refs[NQ + NZ :]
    fill(q_all, q_refs)
    for s in range(NZ):
        vt[:, s * ROWS : (s + 1) * ROWS] = kv[s][:, D:].T
    lse_ref[...] = jnp.zeros(lse_ref.shape, F32)

    def tile(i, carry):
        h, a = i // NY, i % NY
        q = pair(q_all, a, h)
        limits = tile_limits(where, a)
        tops, totals, values = [], [], []
        for s in range(NZ):
            weights, total, top = slot_weights(where, kv, s, q, limits)
            values.append(dot(vt[:, s * ROWS : (s + 1) * ROWS], weights.astype(BF16), NN))
            tops.append(top)
            totals.append(total)
        factors, lse = slot_factors(tops, totals)
        out = sum(f * v for f, v in zip(factors, values))
        put_tile(mine_ref, partner_ref, a, h, out)
        put_rows(lse_ref, a, h, lse)
        return carry

    lax.fori_loop(0, HQ * NY, tile, 0, unroll=4)
    for b in range(NY):
        partner_ref[b, HQ * D :, :] = packed(lse_ref[NY + b, :HQ, :])


def packed(rows):
    high = rows.astype(BF16)
    rest = rows - high.astype(F32)
    middle = rest.astype(BF16)
    low = (rest - middle.astype(F32)).astype(BF16)
    return jnp.concatenate([high, middle, low, jnp.zeros_like(low)], axis=0)


def unpacked(tile):
    rows = tile.astype(F32)
    return rows[:HQ] + rows[HQ : 2 * HQ] + rows[2 * HQ : 3 * HQ]


def join_kernel(mine, lse_ref, got, *outs):
    for b in range(NY):
        ours, theirs = lse_ref[b, :HQ, :], unpacked(got[b, HQ * D :, :])
        top = jnp.maximum(ours, theirs)
        first, second = jnp.exp2(ours - top), jnp.exp2(theirs - top)
        total = first + second
        first, second = first / total, second / total
        lse = top + jnp.log2(total)
        out = outs[b]
        for h in range(HQ):
            rows = slice(h * D, (h + 1) * D)
            value = mine[b, rows, :] * first[h : h + 1] + got[b, rows, :].astype(F32) * second[
                h : h + 1
            ]
            out[rows, :] = value.astype(out.dtype)
        if b == 0:
            outs[NY][...] = jnp.concatenate([lse, lse], axis=0)
        else:
            out[HQ * D :, :] = packed(lse)


def last_kernel(own, lse_ref, *refs):
    others, out_ref = refs[: NY - 1], refs[NY - 1]
    lses = [lse_ref[:HQ, :]] + [unpacked(r[HQ * D :, :]) for r in others]
    top = lses[0]
    for lse in lses[1:]:
        top = jnp.maximum(top, lse)
    weights = [jnp.exp2(lse - top) for lse in lses]
    total = sum(weights)
    weights = [w / total for w in weights]
    for h in range(HQ):
        rows = slice(h * D, (h + 1) * D)
        value = own[rows, :] * weights[0][h : h + 1]
        for r, w in zip(others, weights[1:]):
            value = value + r[rows, :].astype(F32) * w[h : h + 1]
        out_ref[:, rows] = value.T.astype(out_ref.dtype)


def backward_kernel(where, *refs):
    qg_refs, kv, refs = refs[:NQ], refs[NQ : NQ + NZ], refs[NQ + NZ :]
    stats, (mine_ref, partner_ref), refs = refs[:NY], refs[NY : NY + 2], refs[NY + 2 :]
    kv_refs, (qg_all, rows_ref, kt, dk, dv) = refs[:NZ], refs[NZ:]
    fill(qg_all, qg_refs)
    for s in range(NZ):
        kt[:, s * ROWS : (s + 1) * ROWS] = kv[s][:, :D].T
    for slot in range(NQ):
        parts = []
        for s in range(NY):
            k = slot - slot % NY + (slot - s) % NY
            parts.append((stats[s][k, :HQ, :], stats[s][k, HQ:, :]))
        lse, delta = merged_rows(parts)
        rows_ref[slot, :HQ, :] = lse
        rows_ref[slot, HQ:, :] = delta
    dk[...] = jnp.zeros(dk.shape, F32)
    dv[...] = jnp.zeros(dv.shape, F32)

    def tile(i, carry):
        h, a = i // NY, i % NY
        q = pair(qg_all, a, h)
        g = pair(qg_all, a, HQ + h)
        lse = take_rows(rows_ref, a, h)
        delta = take_rows(rows_ref, a, HQ + h)
        limits = tile_limits(where, a)
        probs, grads = [], []
        for s in range(NZ):
            scores = slot_scores(kv, s, q, limits)
            p = jnp.exp2(scores - (lse - slot_bias(where, s)))
            prob_grad = dot(kv[s][:, D:], g, NT)
            probs.append(p.astype(BF16))
            grads.append((p * (prob_grad - delta)).astype(BF16))
        p = jnp.concatenate(probs, axis=0)
        ds = jnp.concatenate(grads, axis=0)
        dv[...] += dot(p, g, NN)
        dk[...] += dot(ds, q, NN)
        put_tile(mine_ref, partner_ref, a, h, dot(kt[...], ds, NN) * SCALE)
        return carry

    lax.fori_loop(0, HQ * NY, tile, 0, unroll=2)
    for s in range(NZ):
        ref = kv_refs[s]
        rows = slice(s * ROWS, (s + 1) * ROWS)
        ref[:, :D] = (dk[rows, :] * SCALE).astype(ref.dtype)
        ref[:, D:] = dv[rows, :].astype(ref.dtype)


SHARE = FEATURES // (NZ * NQ)
WIDTH = (HQ + 2) * D


CHUNKS = 4


def projection_kernel(tokens_ref, weights_ref, grad_ref, out_ref, heads_ref, kv_ref):
    step = pl.program_id(0)
    term = dot(tokens_ref[...], weights_ref[...], NN)

    @pl.when(step == 0)
    def _():
        out_ref[...] = term

    @pl.when(step > 0)
    def _():
        out_ref[...] += term

    @pl.when(step == CHUNKS - 1)
    def _():
        out = out_ref[...].astype(BF16)
        heads_ref[:, : HQ * D] = out[:, : HQ * D]
        heads_ref[:, HQ * D :] = grad_ref[...]
        kv_ref[...] = out[:, HQ * D :]


def project(tokens, projection, cotangent):
    depth = FEATURES // CHUNKS
    outs = (shaped(F32, ROWS, WIDTH), shaped(BF16, ROWS, 2 * HQ * D), shaped(BF16, ROWS, 2 * D))
    return pl.pallas_call(
        projection_kernel,
        grid=(CHUNKS,),
        out_shape=outs,
        in_specs=[
            pl.BlockSpec((ROWS, depth), lambda i: (0, i)),
            pl.BlockSpec((depth, WIDTH), lambda i: (i, 0)),
            pl.BlockSpec((ROWS, HQ * D), lambda i: (0, 0)),
        ],
        out_specs=[pl.BlockSpec(o.shape, lambda i: (0, 0)) for o in outs],
        compiler_params=pltpu.CompilerParams(vmem_limit_bytes=16 << 20),
    )(tokens, projection, cotangent)


def feature_kernel(where, tokens_ref, *refs):
    outs, by_owner = refs[:NY], refs[NY]
    y, c = where[1], where[2]
    for k in range(NQ):
        cols = [
            tokens_ref[:, (j * NQ + k) * SHARE : (j * NQ + k + 1) * SHARE] for j in range(NZ)
        ]
        by_owner[k] = jnp.concatenate(cols, axis=1)
    for s in range(NY):
        row = (y + s) % NY
        outs[s][0] = by_owner[row * NC + c]
        outs[s][1] = by_owner[row * NC + 1 - c]


def feature_slot(refs, slot):
    return refs[slot][slot // NY]


def weight_kernel(where, *refs):
    features, hq, hkv = refs[:NQ], refs[NQ : 2 * NQ], refs[2 * NQ : 3 * NQ]
    outs, (t_all, h_all, grad) = refs[3 * NQ : 3 * NQ + NZ], refs[3 * NQ + NZ :]
    for slot in range(NQ):
        cols = slice(slot * ROWS, (slot + 1) * ROWS)
        t_all[cols, :] = feature_slot(features, slot)
        h_all[: HQ * D, cols] = hq[slot][...]
        h_all[HQ * D :, cols] = hkv[slot][...].T
    for k in range(HQ + 2):
        rows = slice(k * D, (k + 1) * D)
        grad[:, rows] = dot(h_all[rows, :], t_all[...], NN).T
    for s in range(NZ):
        row = (where[0] - s + NZ) % NZ
        rows = grad[pl.ds(pl.multiple_of(row * SHARE, SHARE), SHARE), :]
        outs[s][...] = rows.astype(outs[s].dtype)


def moved_kernel(where, *refs):
    features, shares = refs[:NQ], refs[NQ : NQ + NZ]
    mine_ref, partner_ref, squares_ref, rows_ref = refs[NQ + NZ :]
    squares = jnp.zeros((8, WIDTH), F32)
    for s in range(NZ):
        row = (where[0] - s + NZ) % NZ
        rows_ref[pl.ds(pl.multiple_of(row * SHARE, SHARE), SHARE), :] = shares[s][...]
        value = jnp.square(shares[s][...].astype(F32))
        for k in range(SHARE // 8):
            squares = squares + value[8 * k : 8 * k + 8]
    squares_ref[...] = jnp.full(squares_ref.shape, jnp.sum(squares), F32)
    for b in range(NY):
        mine_ref[b] = dot(feature_slot(features, b), rows_ref[...], NN)
        partner_ref[b] = dot(feature_slot(features, NY + b), rows_ref[...], NN).astype(BF16)


def renew_kernel(projected, *refs):
    terms, (first, second), outs = refs[:NY], refs[NY : NY + 2], refs[NY + 2 :]
    query_ref, kv_ref, squares_ref = outs
    squares = first[...] + second[...]
    squares_ref[...] = squares
    factor = (0.2 * math.sqrt(GROUPS * WIDTH)) / jnp.sqrt(squares[:1, :])
    for k in range(HQ + 2):
        cols = slice(k * D, (k + 1) * D)
        moved = terms[0][:, cols]
        for t in terms[1:]:
            moved = moved + t[:, cols].astype(F32)
        value = (projected[:, cols] + factor * moved).astype(BF16)
        if k < HQ:
            query_ref[:, cols] = value
        else:
            kv_ref[:, (k - HQ) * D : (k - HQ + 1) * D] = value


def call(kernel, outs, scratch, matmuls, *args):
    vmem = pl.BlockSpec(memory_space=pltpu.VMEM)
    smem = pl.BlockSpec(memory_space=pltpu.SMEM)
    specs = [smem if a.dtype == jnp.int32 else vmem for a in args]
    size = HQ * NQ * ROWS * NZ * ROWS
    work = 2 * matmuls * size * D + (8 * size if matmuls else size)
    return pl.pallas_call(
        kernel,
        out_shape=outs,
        in_specs=specs,
        out_specs=jax.tree.map(lambda _: vmem, outs),
        scratch_shapes=scratch,
        cost_estimate=pl.CostEstimate(
            flops=work, bytes_accessed=1 << 20, transcendentals=size if matmuls else 0
        ),
        compiler_params=pltpu.CompilerParams(vmem_limit_bytes=48 << 20),
    )(*args)


def shaped(dtype, *dims):
    return jax.ShapeDtypeStruct(dims, dtype)


def on_device(tokens, projection, context_cotangent):
    z, y, c = lax.axis_index("z"), lax.axis_index("y"), lax.axis_index("c")
    where = jnp.stack([z, y, c]).astype(jnp.int32)
    rows_all = pltpu.VMEM((NQ, ROWS, HQ * D), BF16)
    both_all = pltpu.VMEM((NQ, ROWS, 2 * HQ * D), BF16)
    keys_all = pltpu.VMEM((D, NZ * ROWS), BF16)
    key_sums = pltpu.VMEM((NZ * ROWS, D), F32)
    stat = shaped(F32, NQ, 2 * HQ, ROWS)

    projected, heads, key_value = project(tokens, projection, context_cotangent)
    key_value = pieces(key_value, "z", NZ)
    heads = gather_yc(heads)

    features = call(
        feature_kernel,
        tuple(shaped(BF16, NC, ROWS, FEATURES // NQ) for _ in range(NY)),
        (pltpu.VMEM((NQ, ROWS, FEATURES // NQ), BF16),),
        0,
        where,
        tokens,
    )
    features = [features[0]] + [shift(features[s], "y", NY, s) for s in range(1, NY)]
    features = features + [swap(f) for f in features]

    stats = call(
        stats_kernel, stat, (both_all,), 2, where, *heads, *key_value
    )
    stats = call(pair_kernel, stat, (), 0, stats, swap(stats))
    stats = pieces(stats, "y", NY)

    outs = (
        shaped(F32, NY, HQ * D, ROWS),
        shaped(BF16, NY, HQ * D, ROWS),
        shaped(F32, ROWS, 2 * D),
    ) + tuple(shaped(BF16, ROWS, 2 * D) for _ in range(NZ - 1))
    mine, partner, *kv_terms = call(
        backward_kernel,
        outs,
        (both_all, pltpu.VMEM((NQ, 2 * HQ, ROWS), F32), keys_all, key_sums, key_sums),
        5,
        where,
        *heads,
        *key_value,
        *stats,
    )
    query_grad = gather_yc(scatter_yc(mine, partner).astype(BF16))
    key_value_grad = gather_yc(sum_to_owner(kv_terms, "z", NZ).astype(BF16))

    grad_terms = call(
        weight_kernel,
        (shaped(F32, SHARE, WIDTH),) + tuple(shaped(BF16, SHARE, WIDTH) for _ in range(NZ - 1)),
        (
            pltpu.VMEM((NQ * ROWS, FEATURES // NQ), BF16),
            pltpu.VMEM((WIDTH, NQ * ROWS), BF16),
            pltpu.VMEM((FEATURES // NQ, WIDTH), F32),
        ),
        0,
        where,
        *features,
        *query_grad,
        *key_value_grad,
    )
    own_grad = sum_to_owner(grad_terms, "z", NZ)

    mine, partner, squares = call(
        moved_kernel,
        (
            shaped(F32, NY, ROWS, WIDTH),
            shaped(BF16, NY, ROWS, WIDTH),
            shaped(F32, 8, 128),
        ),
        (pltpu.VMEM((FEATURES // NQ, WIDTH), BF16),),
        0,
        where,
        *features,
        *pieces(own_grad.astype(BF16), "z", NZ),
    )
    moved_rows = mine + swap(partner).astype(F32)
    squares = sum(pieces(squares, "y", NY))
    squares = sum(pieces(squares, "head", GROUPS))
    moved_terms = [moved_rows[0]] + [
        shift(moved_rows[s].astype(BF16), "y", NY, -s) for s in range(1, NY)
    ]
    query_new, key_value_new, squares = call(
        renew_kernel,
        (shaped(BF16, ROWS, HQ * D), shaped(BF16, ROWS, 2 * D), shaped(F32, 8, 128)),
        (),
        0,
        projected,
        *moved_terms,
        squares,
        swap(squares),
    )
    direction = own_grad * (math.sqrt(FEATURES * GROUPS * WIDTH) / jnp.sqrt(squares[0, 0]))
    key_value_new = pieces(key_value_new, "z", NZ)
    query_new = gather_yc(query_new)
    pack = HQ * D + 4 * HQ
    mine, partner, lse = call(
        forward_kernel,
        (shaped(F32, NY, HQ * D, ROWS), shaped(BF16, NY, pack, ROWS), stat),
        (rows_all, keys_all),
        2,
        where,
        *query_new,
        *key_value_new,
    )
    own, *others, lse = call(
        join_kernel,
        (shaped(F32, HQ * D, ROWS),)
        + tuple(shaped(BF16, pack, ROWS) for _ in range(NY - 1))
        + (shaped(F32, 2 * HQ, ROWS),),
        (),
        0,
        mine,
        lse,
        swap(partner),
    )
    others = [shift(others[s - 1], "y", NY, -s) for s in range(1, NY)]
    perturbed = call(last_kernel, shaped(BF16, ROWS, HQ * D), (), 0, own, lse, *others)
    return (perturbed, direction)


def solution(mesh):
    finer = Mesh(mesh.devices.reshape(NZ, NY, NC, GROUPS), ("z", "y", "c", "head"))
    seq = ("z", "y", "c")

    return jax.shard_map(
        on_device,
        mesh=finer,
        in_specs=(P(seq, None), P(None, "head"), P(seq, "head")),
        out_specs=(P(seq, "head"), P(seq, "head")),
        check_vma=False,
    )
```

```python
import math

import jax
import jax.numpy as jnp
from jax import lax
from jax.experimental import pallas as pl
from jax.experimental.pallas import tpu as pltpu
from jax.sharding import Mesh
from jax.sharding import PartitionSpec as P


FEATURES = 2048
GROUPS = 4
D = 128
HQ = 4
ROWS = 128
NY = 4
NC = 2
NZ = 8
NQ = NY * NC
SCALE = D ** (-0.5)
SCALE2 = SCALE * math.log2(math.e)
MASKED = -1e30
FLOOR = -1e29
F32 = jnp.float32
BF16 = jnp.bfloat16
NT = (((1,), (1,)), ((), ()))
NN = (((1,), (0,)), ((), ()))


def shift(x, axis, size, step):
    return lax.ppermute(x, axis, [(j, (j + step) % size) for j in range(size)])


def swap(x):
    return shift(x, "c", NC, 1)


def pieces(x, axis, size):
    return [x] + [shift(x, axis, size, s) for s in range(1, size)]


def ring_z(x):
    slots = [x] + [None] * (NZ - 1)
    for s in range(1, NZ // 2 + 1):
        slots[s] = shift(slots[s - 1], "z", NZ, 1)
    for s in range(1, NZ // 2):
        slots[NZ - s] = shift(slots[(NZ - s + 1) % NZ], "z", NZ, -1)
    return slots


def gather_yc(x):
    mine = pieces(x, "y", NY)
    return mine + [swap(m) for m in mine]


def sum_to_owner(terms, axis, size):
    total = terms[0].astype(F32)
    for s in range(1, size):
        total = total + shift(terms[s].astype(BF16), axis, size, -s).astype(F32)
    return total


def scatter_yc(mine, partner):
    total = mine + swap(partner).astype(F32)
    return sum_to_owner([total[s] for s in range(NY)], "y", NY)


def dot(a, b, dims):
    return lax.dot_general(a, b, dims, preferred_element_type=F32)


def tile_limits(where, a):
    y, c = where[1], where[2]
    lane = lax.broadcasted_iota(jnp.int32, (1, 2 * ROWS), 1)

    def limit(slot):
        other = ((y - slot % NY + NY) % NY) * NC + (c + slot // NY) % NC
        return jnp.where(other > y * NC + c, ROWS, -1)

    first = jnp.where(a == 0, lane, limit(2 * a))
    return jnp.where(lane < ROWS, first, limit(2 * a + 1))


def pair(ref, a, h):
    block = ref[pl.ds(2 * a, 2), :, pl.ds(pl.multiple_of(h * D, D), D)]
    return block.reshape(2 * ROWS, D)


def slot_scores(kv, s, q, limits):
    scores = dot(kv[s][:, :D], q, NT) * SCALE2
    if s == 0:
        row = lax.broadcasted_iota(jnp.int32, scores.shape, 0)
        scores = jnp.where(row <= limits, scores, MASKED)
    return scores


def slot_bias(where, s):
    if s == 0:
        return jnp.float32(0.0)
    return jnp.where(s <= where[0], jnp.float32(0.0), jnp.float32(MASKED))


def slot_weights(where, kv, s, q, limits):
    scores = slot_scores(kv, s, q, limits)
    top = jnp.maximum(jnp.max(scores, axis=0, keepdims=True), FLOOR)
    weights = jnp.exp2(scores - top)
    total = jnp.sum(weights, axis=0, keepdims=True)
    return weights, total, top + slot_bias(where, s)


def slot_factors(tops, totals):
    top = tops[0]
    for t in tops[1:]:
        top = jnp.maximum(top, t)
    factors = [jnp.exp2(t - top) for t in tops]
    total = sum(f * t for f, t in zip(factors, totals))
    safe = jnp.maximum(total, 1e-30)
    lse = jnp.where(total > 0.0, top + jnp.log2(safe), MASKED)
    inverse = 1.0 / safe
    return [f * inverse for f in factors], lse


def put_rows(ref, a, h, row):
    ref[2 * a, pl.ds(h, 1), :] = row[:, :ROWS]
    ref[2 * a + 1, pl.ds(h, 1), :] = row[:, ROWS:]


def take_rows(ref, a, h):
    rows = [ref[2 * a + j, pl.ds(h, 1), :] for j in range(2)]
    return jnp.concatenate(rows, axis=1)


def fill(scratch, refs):
    for s, ref in enumerate(refs):
        scratch[s] = ref[...]


def put_tile(mine_ref, partner_ref, a, h, out):
    rows = pl.ds(pl.multiple_of(h * D, D), D)

    def put(ref, b):
        ref[b, rows, :] = out[:, :ROWS].astype(ref.dtype)
        ref[b + 1, rows, :] = out[:, ROWS:].astype(ref.dtype)

    @pl.when(a < 2)
    def _():
        put(mine_ref, 2 * a)

    @pl.when(a >= 2)
    def _():
        put(partner_ref, 2 * a - NY)


def stats_kernel(where, *refs):
    qg_refs, kv = refs[:NQ], refs[NQ : NQ + NZ]
    out_ref, qg_all = refs[NQ + NZ :]
    fill(qg_all, qg_refs)

    def tile(i, carry):
        h, a = i // NY, i % NY
        q = pair(qg_all, a, h)
        g = pair(qg_all, a, HQ + h)
        limits = tile_limits(where, a)
        tops, totals, values = [], [], []
        for s in range(NZ):
            weights, total, top = slot_weights(where, kv, s, q, limits)
            prob_grad = dot(kv[s][:, D:], g, NT)
            values.append(jnp.sum(weights * prob_grad, axis=0, keepdims=True))
            tops.append(top)
            totals.append(total)
        factors, lse = slot_factors(tops, totals)
        put_rows(out_ref, a, h, lse)
        put_rows(out_ref, a, HQ + h, sum(f * v for f, v in zip(factors, values)))
        return carry

    lax.fori_loop(0, HQ * NY, tile, 0, unroll=4)


def merged_rows(parts):
    top = parts[0][0]
    for lse, _ in parts[1:]:
        top = jnp.maximum(top, lse)
    weights = [jnp.exp2(lse - top) for lse, _ in parts]
    total = sum(weights)
    value = sum(w * v for w, (_, v) in zip(weights, parts)) / total
    return top + jnp.log2(total), value


def pair_kernel(own, got, out_ref):
    for slot in range(NQ):
        other = (slot + NY) % NQ
        lse, delta = merged_rows(
            [(r[k, :HQ, :], r[k, HQ:, :]) for r, k in ((own, slot), (got, other))]
        )
        out_ref[slot, :HQ, :] = lse
        out_ref[slot, HQ:, :] = delta


def forward_kernel(where, *refs):
    q_refs, kv = refs[:NQ], refs[NQ : NQ + NZ]
    mine_ref, partner_ref, lse_ref, q_all, vt = refs[NQ + NZ :]
    fill(q_all, q_refs)
    for s in range(NZ):
        vt[:, s * ROWS : (s + 1) * ROWS] = kv[s][:, D:].T
    lse_ref[...] = jnp.zeros(lse_ref.shape, F32)

    def tile(i, carry):
        h, a = i // NY, i % NY
        q = pair(q_all, a, h)
        limits = tile_limits(where, a)
        tops, totals, values = [], [], []
        for s in range(NZ):
            weights, total, top = slot_weights(where, kv, s, q, limits)
            values.append(dot(vt[:, s * ROWS : (s + 1) * ROWS], weights.astype(BF16), NN))
            tops.append(top)
            totals.append(total)
        factors, lse = slot_factors(tops, totals)
        out = sum(f * v for f, v in zip(factors, values))
        put_tile(mine_ref, partner_ref, a, h, out)
        put_rows(lse_ref, a, h, lse)
        return carry

    lax.fori_loop(0, HQ * NY, tile, 0, unroll=4)
    for b in range(NY):
        partner_ref[b, HQ * D :, :] = packed(lse_ref[NY + b, :HQ, :])


def packed(rows):
    high = rows.astype(BF16)
    rest = rows - high.astype(F32)
    middle = rest.astype(BF16)
    low = (rest - middle.astype(F32)).astype(BF16)
    return jnp.concatenate([high, middle, low, jnp.zeros_like(low)], axis=0)


def unpacked(tile):
    rows = tile.astype(F32)
    return rows[:HQ] + rows[HQ : 2 * HQ] + rows[2 * HQ : 3 * HQ]


def join_kernel(mine, lse_ref, got, *outs):
    for b in range(NY):
        ours, theirs = lse_ref[b, :HQ, :], unpacked(got[b, HQ * D :, :])
        top = jnp.maximum(ours, theirs)
        first, second = jnp.exp2(ours - top), jnp.exp2(theirs - top)
        total = first + second
        first, second = first / total, second / total
        lse = top + jnp.log2(total)
        out = outs[b]
        for h in range(HQ):
            rows = slice(h * D, (h + 1) * D)
            value = mine[b, rows, :] * first[h : h + 1] + got[b, rows, :].astype(F32) * second[
                h : h + 1
            ]
            out[rows, :] = value.astype(out.dtype)
        if b == 0:
            outs[NY][...] = jnp.concatenate([lse, lse], axis=0)
        else:
            out[HQ * D :, :] = packed(lse)


def last_kernel(own, lse_ref, *refs):
    others, out_ref = refs[: NY - 1], refs[NY - 1]
    lses = [lse_ref[:HQ, :]] + [unpacked(r[HQ * D :, :]) for r in others]
    top = lses[0]
    for lse in lses[1:]:
        top = jnp.maximum(top, lse)
    weights = [jnp.exp2(lse - top) for lse in lses]
    total = sum(weights)
    weights = [w / total for w in weights]
    for h in range(HQ):
        rows = slice(h * D, (h + 1) * D)
        value = own[rows, :] * weights[0][h : h + 1]
        for r, w in zip(others, weights[1:]):
            value = value + r[rows, :].astype(F32) * w[h : h + 1]
        out_ref[:, rows] = value.T.astype(out_ref.dtype)


def backward_kernel(where, *refs):
    qg_refs, kv, refs = refs[:NQ], refs[NQ : NQ + NZ], refs[NQ + NZ :]
    stats, (mine_ref, partner_ref), refs = refs[:NY], refs[NY : NY + 2], refs[NY + 2 :]
    kv_refs, (qg_all, rows_ref, kt, dk, dv) = refs[:NZ], refs[NZ:]
    fill(qg_all, qg_refs)
    for s in range(NZ):
        kt[:, s * ROWS : (s + 1) * ROWS] = kv[s][:, :D].T
    for slot in range(NQ):
        parts = []
        for s in range(NY):
            k = slot - slot % NY + (slot - s) % NY
            parts.append((stats[s][k, :HQ, :], stats[s][k, HQ:, :]))
        lse, delta = merged_rows(parts)
        rows_ref[slot, :HQ, :] = lse
        rows_ref[slot, HQ:, :] = delta
    dk[...] = jnp.zeros(dk.shape, F32)
    dv[...] = jnp.zeros(dv.shape, F32)

    def tile(i, carry):
        h, a = i // NY, i % NY
        q = pair(qg_all, a, h)
        g = pair(qg_all, a, HQ + h)
        lse = take_rows(rows_ref, a, h)
        delta = take_rows(rows_ref, a, HQ + h)
        limits = tile_limits(where, a)
        probs, grads = [], []
        for s in range(NZ):
            scores = slot_scores(kv, s, q, limits)
            p = jnp.exp2(scores - (lse - slot_bias(where, s)))
            prob_grad = dot(kv[s][:, D:], g, NT)
            probs.append(p.astype(BF16))
            grads.append((p * (prob_grad - delta)).astype(BF16))
        p = jnp.concatenate(probs, axis=0)
        ds = jnp.concatenate(grads, axis=0)
        dv[...] += dot(p, g, NN)
        dk[...] += dot(ds, q, NN)
        put_tile(mine_ref, partner_ref, a, h, dot(kt[...], ds, NN) * SCALE)
        return carry

    lax.fori_loop(0, HQ * NY, tile, 0, unroll=2)
    for s in range(NZ):
        ref = kv_refs[s]
        rows = slice(s * ROWS, (s + 1) * ROWS)
        ref[:, :D] = (dk[rows, :] * SCALE).astype(ref.dtype)
        ref[:, D:] = dv[rows, :].astype(ref.dtype)


SHARE = FEATURES // (NZ * NQ)
WIDTH = (HQ + 2) * D


def projection_kernel(tokens_ref, weights_ref, grad_ref, out_ref, heads_ref, kv_ref):
    out = dot(tokens_ref[...], weights_ref[...], NN)
    out_ref[...] = out
    heads_ref[:, : HQ * D] = out[:, : HQ * D].astype(BF16)
    heads_ref[:, HQ * D :] = grad_ref[...]
    kv_ref[...] = out[:, HQ * D :].astype(BF16)


def feature_kernel(where, tokens_ref, *refs):
    outs, by_owner = refs[:NY], refs[NY]
    y, c = where[1], where[2]
    for k in range(NQ):
        cols = [
            tokens_ref[:, (j * NQ + k) * SHARE : (j * NQ + k + 1) * SHARE] for j in range(NZ)
        ]
        by_owner[k] = jnp.concatenate(cols, axis=1)
    for s in range(NY):
        row = (y + s) % NY
        outs[s][0] = by_owner[row * NC + c]
        outs[s][1] = by_owner[row * NC + 1 - c]


def feature_slot(refs, slot):
    return refs[slot][slot // NY]


def bundle_kernel(*refs):
    hq, hkv, out_ref = refs[:NY], refs[NY : 2 * NY], refs[2 * NY]
    for b in range(NY):
        out_ref[b, : HQ * D, :] = hq[b][...]
        out_ref[b, HQ * D :, :] = hkv[b][...].T


def weight_kernel(where, *refs):
    features, bundles, refs = refs[:NQ], refs[NQ : NQ + NC], refs[NQ + NC :]
    outs, (t_all, h_all, grad) = refs[:NZ], refs[NZ:]
    for slot in range(NQ):
        cols = slice(slot * ROWS, (slot + 1) * ROWS)
        t_all[cols, :] = feature_slot(features, slot)
        h_all[:, cols] = bundles[slot // NY][slot % NY]
    for k in range(HQ + 2):
        rows = slice(k * D, (k + 1) * D)
        grad[:, rows] = dot(h_all[rows, :], t_all[...], NN).T
    for s in range(NZ):
        row = (where[0] - s + NZ) % NZ
        rows = grad[pl.ds(pl.multiple_of(row * SHARE, SHARE), SHARE), :]
        outs[s][...] = rows.astype(outs[s].dtype)


def moved_kernel(where, *refs):
    features, shares = refs[:NQ], refs[NQ : NQ + NZ]
    mine_ref, partner_ref, squares_ref, rows_ref = refs[NQ + NZ :]
    squares = jnp.zeros((8, WIDTH), F32)
    for s in range(NZ):
        row = (where[0] - s + NZ) % NZ
        rows_ref[pl.ds(pl.multiple_of(row * SHARE, SHARE), SHARE), :] = shares[s][...]
        value = jnp.square(shares[s][...].astype(F32))
        for k in range(SHARE // 8):
            squares = squares + value[8 * k : 8 * k + 8]
    squares_ref[...] = jnp.full(squares_ref.shape, jnp.sum(squares), F32)
    for b in range(NY):
        mine_ref[b] = dot(feature_slot(features, b), rows_ref[...], NN)
        partner_ref[b] = dot(feature_slot(features, NY + b), rows_ref[...], NN).astype(BF16)


def renew_kernel(projected, *refs):
    terms, (first, second), outs = refs[:NY], refs[NY : NY + 2], refs[NY + 2 :]
    query_ref, kv_ref, squares_ref = outs
    squares = first[...] + second[...]
    squares_ref[...] = squares
    factor = (0.2 * math.sqrt(GROUPS * WIDTH)) / jnp.sqrt(squares[:1, :])
    for k in range(HQ + 2):
        cols = slice(k * D, (k + 1) * D)
        moved = terms[0][:, cols]
        for t in terms[1:]:
            moved = moved + t[:, cols].astype(F32)
        value = (projected[:, cols] + factor * moved).astype(BF16)
        if k < HQ:
            query_ref[:, cols] = value
        else:
            kv_ref[:, (k - HQ) * D : (k - HQ + 1) * D] = value


def call(kernel, outs, scratch, matmuls, *args):
    vmem = pl.BlockSpec(memory_space=pltpu.VMEM)
    smem = pl.BlockSpec(memory_space=pltpu.SMEM)
    specs = [smem if a.dtype == jnp.int32 else vmem for a in args]
    size = HQ * NQ * ROWS * NZ * ROWS
    work = 2 * matmuls * size * D + (8 * size if matmuls else size)
    return pl.pallas_call(
        kernel,
        out_shape=outs,
        in_specs=specs,
        out_specs=jax.tree.map(lambda _: vmem, outs),
        scratch_shapes=scratch,
        cost_estimate=pl.CostEstimate(
            flops=work, bytes_accessed=1 << 20, transcendentals=size if matmuls else 0
        ),
        compiler_params=pltpu.CompilerParams(vmem_limit_bytes=48 << 20),
    )(*args)


def shaped(dtype, *dims):
    return jax.ShapeDtypeStruct(dims, dtype)


def on_device(tokens, projection, context_cotangent):
    z, y, c = lax.axis_index("z"), lax.axis_index("y"), lax.axis_index("c")
    where = jnp.stack([z, y, c]).astype(jnp.int32)
    rows_all = pltpu.VMEM((NQ, ROWS, HQ * D), BF16)
    both_all = pltpu.VMEM((NQ, ROWS, 2 * HQ * D), BF16)
    keys_all = pltpu.VMEM((D, NZ * ROWS), BF16)
    key_sums = pltpu.VMEM((NZ * ROWS, D), F32)
    stat = shaped(F32, NQ, 2 * HQ, ROWS)

    projected, heads, key_value = call(
        projection_kernel,
        (shaped(F32, ROWS, WIDTH), shaped(BF16, ROWS, 2 * HQ * D), shaped(BF16, ROWS, 2 * D)),
        (),
        0,
        tokens,
        projection,
        context_cotangent,
    )
    key_value = ring_z(key_value)
    heads = gather_yc(heads)

    features = call(
        feature_kernel,
        tuple(shaped(BF16, NC, ROWS, FEATURES // NQ) for _ in range(NY)),
        (pltpu.VMEM((NQ, ROWS, FEATURES // NQ), BF16),),
        0,
        where,
        tokens,
    )
    features = [features[0]] + [shift(features[s], "y", NY, s) for s in range(1, NY)]
    features = features + [swap(f) for f in features]

    stats = call(
        stats_kernel, stat, (both_all,), 2, where, *heads, *key_value
    )
    stats = call(pair_kernel, stat, (), 0, stats, swap(stats))
    stats = pieces(stats, "y", NY)

    outs = (
        shaped(F32, NY, HQ * D, ROWS),
        shaped(BF16, NY, HQ * D, ROWS),
        shaped(F32, ROWS, 2 * D),
    ) + tuple(shaped(BF16, ROWS, 2 * D) for _ in range(NZ - 1))
    mine, partner, *kv_terms = call(
        backward_kernel,
        outs,
        (both_all, pltpu.VMEM((NQ, 2 * HQ, ROWS), F32), keys_all, key_sums, key_sums),
        5,
        where,
        *heads,
        *key_value,
        *stats,
    )
    query_grad = scatter_yc(mine, partner).astype(BF16)
    key_value_grad = sum_to_owner(kv_terms, "z", NZ).astype(BF16)
    bundle = call(
        bundle_kernel,
        shaped(BF16, NY, WIDTH, ROWS),
        (),
        0,
        *pieces(query_grad, "y", NY),
        *pieces(key_value_grad, "y", NY),
    )

    grad_terms = call(
        weight_kernel,
        (shaped(F32, SHARE, WIDTH),) + tuple(shaped(BF16, SHARE, WIDTH) for _ in range(NZ - 1)),
        (
            pltpu.VMEM((NQ * ROWS, FEATURES // NQ), BF16),
            pltpu.VMEM((WIDTH, NQ * ROWS), BF16),
            pltpu.VMEM((FEATURES // NQ, WIDTH), F32),
        ),
        0,
        where,
        *features,
        bundle,
        swap(bundle),
    )
    own_grad = sum_to_owner(grad_terms, "z", NZ)

    mine, partner, squares = call(
        moved_kernel,
        (
            shaped(F32, NY, ROWS, WIDTH),
            shaped(BF16, NY, ROWS, WIDTH),
            shaped(F32, 8, 128),
        ),
        (pltpu.VMEM((FEATURES // NQ, WIDTH), BF16),),
        0,
        where,
        *features,
        *pieces(own_grad.astype(BF16), "z", NZ),
    )
    moved_rows = mine + swap(partner).astype(F32)
    squares = sum(pieces(squares, "y", NY))
    squares = sum(pieces(squares, "head", GROUPS))
    moved_terms = [moved_rows[0]] + [
        shift(moved_rows[s].astype(BF16), "y", NY, -s) for s in range(1, NY)
    ]
    query_new, key_value_new, squares = call(
        renew_kernel,
        (shaped(BF16, ROWS, HQ * D), shaped(BF16, ROWS, 2 * D), shaped(F32, 8, 128)),
        (),
        0,
        projected,
        *moved_terms,
        squares,
        swap(squares),
    )
    direction = own_grad * (math.sqrt(FEATURES * GROUPS * WIDTH) / jnp.sqrt(squares[0, 0]))
    key_value_new = ring_z(key_value_new)
    query_new = gather_yc(query_new)
    pack = HQ * D + 4 * HQ
    mine, partner, lse = call(
        forward_kernel,
        (shaped(F32, NY, HQ * D, ROWS), shaped(BF16, NY, pack, ROWS), stat),
        (rows_all, keys_all),
        2,
        where,
        *query_new,
        *key_value_new,
    )
    own, *others, lse = call(
        join_kernel,
        (shaped(F32, HQ * D, ROWS),)
        + tuple(shaped(BF16, pack, ROWS) for _ in range(NY - 1))
        + (shaped(F32, 2 * HQ, ROWS),),
        (),
        0,
        mine,
        lse,
        swap(partner),
    )
    others = [shift(others[s - 1], "y", NY, -s) for s in range(1, NY)]
    perturbed = call(last_kernel, shaped(BF16, ROWS, HQ * D), (), 0, own, lse, *others)
    return (perturbed, direction)


def solution(mesh):
    finer = Mesh(mesh.devices.reshape(NZ, NY, NC, GROUPS), ("z", "y", "c", "head"))
    seq = ("z", "y", "c")

    return jax.shard_map(
        on_device,
        mesh=finer,
        in_specs=(P(seq, None), P(None, "head"), P(seq, "head")),
        out_specs=(P(seq, "head"), P(seq, "head")),
        check_vma=False,
    )
```

```python
import math

import jax
import jax.numpy as jnp
from jax import lax
from jax.experimental import pallas as pl
from jax.experimental.pallas import tpu as pltpu
from jax.sharding import Mesh
from jax.sharding import PartitionSpec as P


FEATURES = 2048
GROUPS = 4
D = 128
HQ = 4
ROWS = 128
NY = 4
NC = 2
NZ = 8
NQ = NY * NC
SCALE = D ** (-0.5)
SCALE2 = SCALE * math.log2(math.e)
MASKED = -1e30
FLOOR = -1e29
F32 = jnp.float32
BF16 = jnp.bfloat16
NT = (((1,), (1,)), ((), ()))
NN = (((1,), (0,)), ((), ()))


def shift(x, axis, size, step):
    return lax.ppermute(x, axis, [(j, (j + step) % size) for j in range(size)])


def swap(x):
    return shift(x, "c", NC, 1)


def pieces(x, axis, size):
    return [x] + [shift(x, axis, size, s) for s in range(1, size)]


def gather_yc(x):
    mine = pieces(x, "y", NY)
    return mine + [swap(m) for m in mine]


def sum_to_owner(terms, axis, size):
    total = terms[0].astype(F32)
    for s in range(1, size):
        total = total + shift(terms[s].astype(BF16), axis, size, -s).astype(F32)
    return total


def scatter_yc(mine, partner):
    total = mine + swap(partner).astype(F32)
    return sum_to_owner([total[s] for s in range(NY)], "y", NY)


def dot(a, b, dims):
    return lax.dot_general(a, b, dims, preferred_element_type=F32)


def tile_limits(where, a):
    y, c = where[1], where[2]
    lane = lax.broadcasted_iota(jnp.int32, (1, 2 * ROWS), 1)

    def limit(slot):
        other = ((y - slot % NY + NY) % NY) * NC + (c + slot // NY) % NC
        return jnp.where(other > y * NC + c, ROWS, -1)

    first = jnp.where(a == 0, lane, limit(2 * a))
    return jnp.where(lane < ROWS, first, limit(2 * a + 1))


def pair(ref, a, h):
    block = ref[pl.ds(2 * a, 2), :, pl.ds(pl.multiple_of(h * D, D), D)]
    return block.reshape(2 * ROWS, D)


def slot_scores(kv, s, q, limits):
    scores = dot(kv[s][:, :D], q, NT) * SCALE2
    if s == 0:
        row = lax.broadcasted_iota(jnp.int32, scores.shape, 0)
        scores = jnp.where(row <= limits, scores, MASKED)
    return scores


def slot_bias(where, s):
    if s == 0:
        return jnp.float32(0.0)
    return jnp.where(s <= where[0], jnp.float32(0.0), jnp.float32(MASKED))


def slot_weights(where, kv, s, q, limits):
    scores = slot_scores(kv, s, q, limits)
    top = jnp.maximum(jnp.max(scores, axis=0, keepdims=True), FLOOR)
    weights = jnp.exp2(scores - top)
    total = jnp.sum(weights, axis=0, keepdims=True)
    return weights, total, top + slot_bias(where, s)


def slot_factors(tops, totals):
    top = tops[0]
    for t in tops[1:]:
        top = jnp.maximum(top, t)
    factors = [jnp.exp2(t - top) for t in tops]
    total = sum(f * t for f, t in zip(factors, totals))
    safe = jnp.maximum(total, 1e-30)
    lse = jnp.where(total > 0.0, top + jnp.log2(safe), MASKED)
    inverse = 1.0 / safe
    return [f * inverse for f in factors], lse


def put_rows(ref, a, h, row):
    ref[2 * a, pl.ds(h, 1), :] = row[:, :ROWS]
    ref[2 * a + 1, pl.ds(h, 1), :] = row[:, ROWS:]


def take_rows(ref, a, h):
    rows = [ref[2 * a + j, pl.ds(h, 1), :] for j in range(2)]
    return jnp.concatenate(rows, axis=1)


def fill(scratch, refs):
    for s, ref in enumerate(refs):
        scratch[s] = ref[...]


def put_tile(mine_ref, partner_ref, a, h, out):
    rows = pl.ds(pl.multiple_of(h * D, D), D)

    def put(ref, b):
        ref[b, rows, :] = out[:, :ROWS].astype(ref.dtype)
        ref[b + 1, rows, :] = out[:, ROWS:].astype(ref.dtype)

    @pl.when(a < 2)
    def _():
        put(mine_ref, 2 * a)

    @pl.when(a >= 2)
    def _():
        put(partner_ref, 2 * a - NY)


def stats_kernel(where, *refs):
    qg_refs, kv = refs[:NQ], refs[NQ : NQ + NZ]
    out_ref, qg_all = refs[NQ + NZ :]
    fill(qg_all, qg_refs)

    def tile(i, carry):
        h, a = i // NY, i % NY
        q = pair(qg_all, a, h)
        g = pair(qg_all, a, HQ + h)
        limits = tile_limits(where, a)
        tops, totals, values = [], [], []
        for s in range(NZ):
            weights, total, top = slot_weights(where, kv, s, q, limits)
            prob_grad = dot(kv[s][:, D:], g, NT)
            values.append(jnp.sum(weights * prob_grad, axis=0, keepdims=True))
            tops.append(top)
            totals.append(total)
        factors, lse = slot_factors(tops, totals)
        put_rows(out_ref, a, h, lse)
        put_rows(out_ref, a, HQ + h, sum(f * v for f, v in zip(factors, values)))
        return carry

    lax.fori_loop(0, HQ * NY, tile, 0, unroll=4)


def merged_rows(parts):
    top = parts[0][0]
    for lse, _ in parts[1:]:
        top = jnp.maximum(top, lse)
    weights = [jnp.exp2(lse - top) for lse, _ in parts]
    total = sum(weights)
    value = sum(w * v for w, (_, v) in zip(weights, parts)) / total
    return top + jnp.log2(total), value


def pair_kernel(own, got, out_ref):
    for slot in range(NQ):
        other = (slot + NY) % NQ
        lse, delta = merged_rows(
            [(r[k, :HQ, :], r[k, HQ:, :]) for r, k in ((own, slot), (got, other))]
        )
        out_ref[slot, :HQ, :] = lse
        out_ref[slot, HQ:, :] = delta


def forward_kernel(where, *refs):
    q_refs, kv = refs[:NQ], refs[NQ : NQ + NZ]
    mine_ref, partner_ref, lse_ref, q_all, vt = refs[NQ + NZ :]
    fill(q_all, q_refs)
    for s in range(NZ):
        vt[:, s * ROWS : (s + 1) * ROWS] = kv[s][:, D:].T
    lse_ref[...] = jnp.zeros(lse_ref.shape, F32)

    def tile(i, carry):
        h, a = i // NY, i % NY
        q = pair(q_all, a, h)
        limits = tile_limits(where, a)
        tops, totals, values = [], [], []
        for s in range(NZ):
            weights, total, top = slot_weights(where, kv, s, q, limits)
            values.append(dot(vt[:, s * ROWS : (s + 1) * ROWS], weights.astype(BF16), NN))
            tops.append(top)
            totals.append(total)
        factors, lse = slot_factors(tops, totals)
        out = sum(f * v for f, v in zip(factors, values))
        put_tile(mine_ref, partner_ref, a, h, out)
        put_rows(lse_ref, a, h, lse)
        return carry

    lax.fori_loop(0, HQ * NY, tile, 0, unroll=4)
    for b in range(NY):
        partner_ref[b, HQ * D :, :] = packed(lse_ref[NY + b, :HQ, :])


def packed(rows):
    high = rows.astype(BF16)
    rest = rows - high.astype(F32)
    middle = rest.astype(BF16)
    low = (rest - middle.astype(F32)).astype(BF16)
    return jnp.concatenate([high, middle, low, jnp.zeros_like(low)], axis=0)


def unpacked(tile):
    rows = tile.astype(F32)
    return rows[:HQ] + rows[HQ : 2 * HQ] + rows[2 * HQ : 3 * HQ]


def join_kernel(mine, lse_ref, got, *outs):
    for b in range(NY):
        ours, theirs = lse_ref[b, :HQ, :], unpacked(got[b, HQ * D :, :])
        top = jnp.maximum(ours, theirs)
        first, second = jnp.exp2(ours - top), jnp.exp2(theirs - top)
        total = first + second
        first, second = first / total, second / total
        lse = top + jnp.log2(total)
        out = outs[b]
        for h in range(HQ):
            rows = slice(h * D, (h + 1) * D)
            value = mine[b, rows, :] * first[h : h + 1] + got[b, rows, :].astype(F32) * second[
                h : h + 1
            ]
            out[rows, :] = value.astype(out.dtype)
        if b == 0:
            outs[NY][...] = jnp.concatenate([lse, lse], axis=0)
        else:
            out[HQ * D :, :] = packed(lse)


def last_kernel(own, lse_ref, *refs):
    others, out_ref = refs[: NY - 1], refs[NY - 1]
    lses = [lse_ref[:HQ, :]] + [unpacked(r[HQ * D :, :]) for r in others]
    top = lses[0]
    for lse in lses[1:]:
        top = jnp.maximum(top, lse)
    weights = [jnp.exp2(lse - top) for lse in lses]
    total = sum(weights)
    weights = [w / total for w in weights]
    for h in range(HQ):
        rows = slice(h * D, (h + 1) * D)
        value = own[rows, :] * weights[0][h : h + 1]
        for r, w in zip(others, weights[1:]):
            value = value + r[rows, :].astype(F32) * w[h : h + 1]
        out_ref[:, rows] = value.T.astype(out_ref.dtype)


def backward_kernel(where, *refs):
    qg_refs, kv, refs = refs[:NQ], refs[NQ : NQ + NZ], refs[NQ + NZ :]
    stats, (mine_ref, partner_ref), refs = refs[:NY], refs[NY : NY + 2], refs[NY + 2 :]
    kv_refs, (qg_all, rows_ref, kt, dk, dv) = refs[:NZ], refs[NZ:]
    fill(qg_all, qg_refs)
    for s in range(NZ):
        kt[:, s * ROWS : (s + 1) * ROWS] = kv[s][:, :D].T
    for slot in range(NQ):
        parts = []
        for s in range(NY):
            k = slot - slot % NY + (slot - s) % NY
            parts.append((stats[s][k, :HQ, :], stats[s][k, HQ:, :]))
        lse, delta = merged_rows(parts)
        rows_ref[slot, :HQ, :] = lse
        rows_ref[slot, HQ:, :] = delta
    dk[...] = jnp.zeros(dk.shape, F32)
    dv[...] = jnp.zeros(dv.shape, F32)

    def tile(i, carry):
        h, a = i // NY, i % NY
        q = pair(qg_all, a, h)
        g = pair(qg_all, a, HQ + h)
        lse = take_rows(rows_ref, a, h)
        delta = take_rows(rows_ref, a, HQ + h)
        limits = tile_limits(where, a)
        probs, grads = [], []
        for s in range(NZ):
            scores = slot_scores(kv, s, q, limits)
            p = jnp.exp2(scores - (lse - slot_bias(where, s)))
            prob_grad = dot(kv[s][:, D:], g, NT)
            probs.append(p.astype(BF16))
            grads.append((p * (prob_grad - delta)).astype(BF16))
        p = jnp.concatenate(probs, axis=0)
        ds = jnp.concatenate(grads, axis=0)
        dv[...] += dot(p, g, NN)
        dk[...] += dot(ds, q, NN)
        put_tile(mine_ref, partner_ref, a, h, dot(kt[...], ds, NN) * SCALE)
        return carry

    lax.fori_loop(0, HQ * NY, tile, 0, unroll=2)
    for s in range(NZ):
        ref = kv_refs[s]
        rows = slice(s * ROWS, (s + 1) * ROWS)
        ref[:, :D] = (dk[rows, :] * SCALE).astype(ref.dtype)
        ref[:, D:] = dv[rows, :].astype(ref.dtype)


SHARE = FEATURES // (NZ * NQ)
WIDTH = (HQ + 2) * D


def projection_kernel(tokens_ref, weights_ref, grad_ref, out_ref, heads_ref, kv_ref):
    out = dot(tokens_ref[...], weights_ref[...], NN)
    out_ref[...] = out
    heads_ref[:, : HQ * D] = out[:, : HQ * D].astype(BF16)
    heads_ref[:, HQ * D :] = grad_ref[...]
    kv_ref[...] = out[:, HQ * D :].astype(BF16)


def feature_kernel(where, tokens_ref, *refs):
    outs, by_owner = refs[:NY], refs[NY]
    y, c = where[1], where[2]
    for k in range(NQ):
        cols = [
            tokens_ref[:, (j * NQ + k) * SHARE : (j * NQ + k + 1) * SHARE] for j in range(NZ)
        ]
        by_owner[k] = jnp.concatenate(cols, axis=1)
    for s in range(NY):
        row = (y + s) % NY
        outs[s][0] = by_owner[row * NC + c]
        outs[s][1] = by_owner[row * NC + 1 - c]


def feature_slot(refs, slot):
    return refs[slot][slot // NY]


def weight_kernel(where, *refs):
    features, hq, hkv = refs[:NQ], refs[NQ : 2 * NQ], refs[2 * NQ : 3 * NQ]
    outs, (t_all, h_all, grad) = refs[3 * NQ : 3 * NQ + NZ], refs[3 * NQ + NZ :]
    for slot in range(NQ):
        cols = slice(slot * ROWS, (slot + 1) * ROWS)
        t_all[cols, :] = feature_slot(features, slot)
        h_all[: HQ * D, cols] = hq[slot][...]
        h_all[HQ * D :, cols] = hkv[slot][...].T
    for k in range(HQ + 2):
        rows = slice(k * D, (k + 1) * D)
        grad[:, rows] = dot(h_all[rows, :], t_all[...], NN).T
    for s in range(NZ):
        row = (where[0] - s + NZ) % NZ
        rows = grad[pl.ds(pl.multiple_of(row * SHARE, SHARE), SHARE), :]
        outs[s][...] = rows.astype(outs[s].dtype)


def moved_kernel(where, *refs):
    features, shares = refs[:NQ], refs[NQ : NQ + NZ]
    mine_ref, partner_ref, squares_ref, rows_ref = refs[NQ + NZ :]
    squares = jnp.zeros((8, WIDTH), F32)
    for s in range(NZ):
        row = (where[0] - s + NZ) % NZ
        rows_ref[pl.ds(pl.multiple_of(row * SHARE, SHARE), SHARE), :] = shares[s][...]
        value = jnp.square(shares[s][...].astype(F32))
        for k in range(SHARE // 8):
            squares = squares + value[8 * k : 8 * k + 8]
    squares_ref[...] = jnp.full(squares_ref.shape, jnp.sum(squares), F32)
    for b in range(NY):
        mine_ref[b] = dot(feature_slot(features, b), rows_ref[...], NN)
        partner_ref[b] = dot(feature_slot(features, NY + b), rows_ref[...], NN).astype(BF16)


def renew_kernel(projected, *refs):
    terms, parts, outs = refs[:NY], refs[NY : NY + GROUPS], refs[NY + GROUPS :]
    query_ref, kv_ref, squares_ref = outs
    squares = parts[0][...]
    for part in parts[1:]:
        squares = squares + part[...]
    squares_ref[...] = squares
    factor = (0.2 * math.sqrt(GROUPS * WIDTH)) / jnp.sqrt(squares[:1, :])
    for k in range(HQ + 2):
        cols = slice(k * D, (k + 1) * D)
        moved = terms[0][:, cols]
        for t in terms[1:]:
            moved = moved + t[:, cols].astype(F32)
        value = (projected[:, cols] + factor * moved).astype(BF16)
        if k < HQ:
            query_ref[:, cols] = value
        else:
            kv_ref[:, (k - HQ) * D : (k - HQ + 1) * D] = value


def call(kernel, outs, scratch, matmuls, *args):
    vmem = pl.BlockSpec(memory_space=pltpu.VMEM)
    smem = pl.BlockSpec(memory_space=pltpu.SMEM)
    specs = [smem if a.dtype == jnp.int32 else vmem for a in args]
    size = HQ * NQ * ROWS * NZ * ROWS
    work = 2 * matmuls * size * D + (8 * size if matmuls else size)
    return pl.pallas_call(
        kernel,
        out_shape=outs,
        in_specs=specs,
        out_specs=jax.tree.map(lambda _: vmem, outs),
        scratch_shapes=scratch,
        cost_estimate=pl.CostEstimate(
            flops=work, bytes_accessed=1 << 20, transcendentals=size if matmuls else 0
        ),
        compiler_params=pltpu.CompilerParams(vmem_limit_bytes=48 << 20),
    )(*args)


def shaped(dtype, *dims):
    return jax.ShapeDtypeStruct(dims, dtype)


def on_device(tokens, projection, context_cotangent):
    z, y, c = lax.axis_index("z"), lax.axis_index("y"), lax.axis_index("c")
    where = jnp.stack([z, y, c]).astype(jnp.int32)
    rows_all = pltpu.VMEM((NQ, ROWS, HQ * D), BF16)
    both_all = pltpu.VMEM((NQ, ROWS, 2 * HQ * D), BF16)
    keys_all = pltpu.VMEM((D, NZ * ROWS), BF16)
    key_sums = pltpu.VMEM((NZ * ROWS, D), F32)
    stat = shaped(F32, NQ, 2 * HQ, ROWS)

    projected, heads, key_value = call(
        projection_kernel,
        (shaped(F32, ROWS, WIDTH), shaped(BF16, ROWS, 2 * HQ * D), shaped(BF16, ROWS, 2 * D)),
        (),
        0,
        tokens,
        projection,
        context_cotangent,
    )
    key_value = pieces(key_value, "z", NZ)
    heads = gather_yc(heads)

    features = call(
        feature_kernel,
        tuple(shaped(BF16, NC, ROWS, FEATURES // NQ) for _ in range(NY)),
        (pltpu.VMEM((NQ, ROWS, FEATURES // NQ), BF16),),
        0,
        where,
        tokens,
    )
    features = [features[0]] + [shift(features[s], "y", NY, s) for s in range(1, NY)]
    features = features + [swap(f) for f in features]

    stats = call(
        stats_kernel, stat, (both_all,), 2, where, *heads, *key_value
    )
    stats = call(pair_kernel, stat, (), 0, stats, swap(stats))
    stats = pieces(stats, "y", NY)

    outs = (
        shaped(F32, NY, HQ * D, ROWS),
        shaped(BF16, NY, HQ * D, ROWS),
        shaped(F32, ROWS, 2 * D),
    ) + tuple(shaped(BF16, ROWS, 2 * D) for _ in range(NZ - 1))
    mine, partner, *kv_terms = call(
        backward_kernel,
        outs,
        (both_all, pltpu.VMEM((NQ, 2 * HQ, ROWS), F32), keys_all, key_sums, key_sums),
        5,
        where,
        *heads,
        *key_value,
        *stats,
    )
    query_grad = gather_yc(scatter_yc(mine, partner).astype(BF16))
    key_value_grad = gather_yc(sum_to_owner(kv_terms, "z", NZ).astype(BF16))

    grad_terms = call(
        weight_kernel,
        (shaped(F32, SHARE, WIDTH),) + tuple(shaped(BF16, SHARE, WIDTH) for _ in range(NZ - 1)),
        (
            pltpu.VMEM((NQ * ROWS, FEATURES // NQ), BF16),
            pltpu.VMEM((WIDTH, NQ * ROWS), BF16),
            pltpu.VMEM((FEATURES // NQ, WIDTH), F32),
        ),
        0,
        where,
        *features,
        *query_grad,
        *key_value_grad,
    )
    own_grad = sum_to_owner(grad_terms, "z", NZ)

    mine, partner, squares = call(
        moved_kernel,
        (
            shaped(F32, NY, ROWS, WIDTH),
            shaped(BF16, NY, ROWS, WIDTH),
            shaped(F32, 8, 128),
        ),
        (pltpu.VMEM((FEATURES // NQ, WIDTH), BF16),),
        0,
        where,
        *features,
        *pieces(own_grad.astype(BF16), "z", NZ),
    )
    moved_rows = mine + swap(partner).astype(F32)
    squares = squares + swap(squares)
    squares = sum(pieces(squares, "y", NY))
    moved_terms = [moved_rows[0]] + [
        shift(moved_rows[s].astype(BF16), "y", NY, -s) for s in range(1, NY)
    ]
    query_new, key_value_new, squares = call(
        renew_kernel,
        (shaped(BF16, ROWS, HQ * D), shaped(BF16, ROWS, 2 * D), shaped(F32, 8, 128)),
        (),
        0,
        projected,
        *moved_terms,
        *pieces(squares, "head", GROUPS),
    )
    direction = own_grad * (math.sqrt(FEATURES * GROUPS * WIDTH) / jnp.sqrt(squares[0, 0]))
    key_value_new = pieces(key_value_new, "z", NZ)
    query_new = gather_yc(query_new)
    pack = HQ * D + 4 * HQ
    mine, partner, lse = call(
        forward_kernel,
        (shaped(F32, NY, HQ * D, ROWS), shaped(BF16, NY, pack, ROWS), stat),
        (rows_all, keys_all),
        2,
        where,
        *query_new,
        *key_value_new,
    )
    own, *others, lse = call(
        join_kernel,
        (shaped(F32, HQ * D, ROWS),)
        + tuple(shaped(BF16, pack, ROWS) for _ in range(NY - 1))
        + (shaped(F32, 2 * HQ, ROWS),),
        (),
        0,
        mine,
        lse,
        swap(partner),
    )
    others = [shift(others[s - 1], "y", NY, -s) for s in range(1, NY)]
    perturbed = call(last_kernel, shaped(BF16, ROWS, HQ * D), (), 0, own, lse, *others)
    return (perturbed, direction)


def solution(mesh):
    finer = Mesh(mesh.devices.reshape(NZ, NY, NC, GROUPS), ("z", "y", "c", "head"))
    seq = ("z", "y", "c")

    return jax.shard_map(
        on_device,
        mesh=finer,
        in_specs=(P(seq, None), P(None, "head"), P(seq, "head")),
        out_specs=(P(seq, "head"), P(seq, "head")),
        check_vma=False,
    )
```
